32 devices in a mesh: clip: 4 (over z), tm: 8 (over y, x, core).
Axes of the slice: x: 2, y: 2, z: 4, core: 2. Of those that a mesh axis runs over, the one named last changes fastest.
Arguments:
- tokens: bfloat16 [4, 8, 256, 2048], P('clip', 'tm'), may hold values from -16 to 16
- spatial_queries: bfloat16 [4, 8, 256, 1024], P('clip', 'tm'), may hold values from -4.5 to 4.5
- spatial_keys: bfloat16 [4, 8, 256, 1024], P('clip', 'tm'), may hold values from -4.5 to 4.5
- spatial_values: bfloat16 [4, 8, 256, 1024], P('clip', 'tm'), may hold values from -6 to 6
- spatial_proj: bfloat16 [1024, 2048], P('tm'), may hold values from -0.1875 to 0.1875
- temporal_qkv: bfloat16 [2048, 3072], P('tm'), may hold values from -0.13258252 to 0.13258252
- temporal_proj: bfloat16 [1024, 2048], P('tm'), may hold values from -0.1875 to 0.1875
- frame_mask: int32 [4, 8, 8], P('clip'), may hold values from 0 to 1, as said below
- expert_ids: int32 [4, 8, 256, 2], P('clip', 'tm'), may hold values from 0 to 31, all different within a row; in each aligned block of 256 rows (0 to 255, 256 to 511, ..., all dimensions but the last counted through in order) at most 32 rows name the same one
- gate_values: float32 [4, 8, 256, 2], P('clip', 'tm'), may hold values from 0.2 to 1
- expert_gate: bfloat16 [32, 2048, 1408], P(('clip', 'tm')), may hold values from -0.125 to 0.125
- expert_up: bfloat16 [32, 2048, 1408], P(('clip', 'tm')), may hold values from -0.125 to 0.125
- expert_down: bfloat16 [32, 1408, 2048], P(('clip', 'tm')), may hold values from -0.15625 to 0.15625
Outputs:
- layer_out: bfloat16 [4, 8, 256, 2048], P('clip', 'tm')
The draws below stay inside these ranges and needn't reach their ends.
Inputs may be any that keep to these rules, and one draw needn't show every extreme that they name: `expert_ids`: each token names 2 different experts. Among the 256 tokens of one clip and frame, no expert is named by more than 32 tokens, and in some frames one expert is named by exactly 32. frame_mask[c, i, j] is 1 where j = i and 0 where j > i.
All inputs are finite; a program needn't handle non-finite values.
Results may differ from the reference program's by a relative error of at most 0.013.
Values may be sent and summed in bfloat16 or wider, within the bound.
No kernel may reach another device: no remote copies, remote signals or barrier semaphores. Data moves between devices by JAX's collectives and lax.ppermute only.
A program may use at most 128 MiB of HBM per device.

```python
import math
import jax
import jax.numpy as jnp
import numpy as np
from jax import lax

D = 2048
HEADS = 8
HD = 128
FF = 1408
TOP = 2
POS = 256
EXPERTS = 32
CLIPS = 4
FRAMES = 8
HH = 1024
CAP = 32


def draw_tokens(key, part):
    full_shape = (CLIPS, FRAMES, POS, D)
    values = jnp.clip(jax.random.normal(jax.random.fold_in(key, 11), full_shape, jnp.float32), -6.0, 6.0)
    return values.astype(jnp.bfloat16)


def spatial_pair(key):
    base_key = jax.random.fold_in(key, 3131)
    full_shape = (CLIPS, FRAMES, POS, HEADS, HD)
    query_side = jnp.clip(jax.random.normal(jax.random.fold_in(base_key, 1), full_shape, jnp.float32), -4.5, 4.5)
    key_side = jnp.clip(jax.random.normal(jax.random.fold_in(base_key, 2), full_shape, jnp.float32), -4.5, 4.5)
    flat_shape = (CLIPS, FRAMES, POS, HEADS * HD)
    return (query_side.reshape(flat_shape), key_side.reshape(flat_shape))


def draw_spatial_queries(key, part):
    query_side, key_side = spatial_pair(key)
    return query_side.astype(jnp.bfloat16)


def draw_spatial_keys(key, part):
    query_side, key_side = spatial_pair(key)
    return key_side.astype(jnp.bfloat16)


def draw_temporal_qkv(key, part):
    fan_scale = 1.0 / math.sqrt(D)
    full_shape = (D, 3, HEADS, HD)
    values = jax.random.normal(jax.random.fold_in(key, 21), full_shape, jnp.float32) * fan_scale
    values = jnp.clip(values, -6.0 * fan_scale, 6.0 * fan_scale)
    return values.reshape(D, 3 * HEADS * HD).astype(jnp.bfloat16)


def draw_frame_mask(key, part):
    coin_flips = jax.random.randint(jax.random.fold_in(key, 55), (CLIPS, FRAMES, FRAMES), 0, 2)
    row_index = jnp.arange(FRAMES, dtype=jnp.int32)[:, None]
    col_index = jnp.arange(FRAMES, dtype=jnp.int32)[None, :]
    diagonal = jnp.where(col_index == row_index, 1, 0)
    return jnp.where(col_index < row_index, coin_flips, diagonal[None, :, :]).astype(jnp.int32)


def block_levels(own_key, shape, cuts, low, high):
    loudness = 1.0
    for dim, shards_of in cuts:
        draws = jax.random.uniform(jax.random.fold_in(jax.random.fold_in(own_key, 6), dim), (shards_of,), jnp.float32, low / len(cuts), high / len(cuts))
        loudness = loudness * jnp.repeat(jnp.exp(draws), shape[dim] // shards_of).reshape((-1,) + (1,) * (len(shape) - 1 - dim))
    return loudness


def deal_out(key, own, number, rows, number_of, top, reach, lean):
    order = jax.random.permutation(key, number_of)
    heavy_load, common = load_shares(number_of, rows * top, reach, lean, True), load_shares(number_of, rows * top, reach, lean, False)
    places = jnp.arange(number_of)

    def named(tallies, rotation):
        used = int((tallies > 0).sum())
        fixed = max(1, used // 4)
        passed = fixed + (places - fixed + rotation * (used - fixed)) % max(1, number_of - fixed)
        return jnp.zeros((number_of,), jnp.int32).at[order[jnp.where(places < fixed, places, passed)]].set(jnp.asarray(tallies, jnp.int32))

    tallies = jnp.where(number % 4 == 0, named(heavy_load, number // 4), named(common, number - number // 4 - 1))
    mixed = jax.random.permutation(jax.random.fold_in(own, 3), number_of)
    donor, taker = mixed[0:number_of // 2 * 2:2], mixed[1:number_of // 2 * 2:2]
    slack = jnp.minimum(tallies[donor] - 1, reach - tallies[taker]) // 2
    slack = jnp.where((donor == order[0]) | (taker == order[0]) | (tallies[taker] == 0), 0, jnp.maximum(slack, 0))
    passed = jax.random.randint(jax.random.fold_in(own, 4), (number_of // 2,), 0, 1 << 20) % (slack + 1)
    tallies = tallies.at[donor].add(-passed).at[taker].add(passed)
    labels = jnp.searchsorted(jnp.cumsum(tallies), jnp.arange(rows * top), side="right").astype(jnp.int32)
    table = labels.reshape(top, rows).T
    table = table[jax.random.permutation(jax.random.fold_in(own, 1), rows)]
    rotation = jax.random.randint(jax.random.fold_in(own, 2), (rows, 1), 0, top)
    return jnp.take_along_axis(table, (jnp.arange(top)[None, :] + rotation) % top, axis=1)


def load_shares(amount, total, bound, skew, full):
    loads = [(1 << 20) // math.isqrt(grade ** skew) + 1 for grade in range(1, amount + 1)]
    largest = bound if full else min(bound, max(-(-total // amount), total * loads[0] // sum(loads)))
    least = 1 if total - largest >= amount - 1 else 0
    given, spare = [largest] + [least] * (amount - 1), total - largest - least * (amount - 1)
    while spare > 0:
        movable = [i for i in range(1, amount) if given[i] < largest] or [i for i in range(1, amount) if given[i] < bound]
        whole, left = sum([loads[i] for i in movable]), spare
        for i in movable:
            more = min(bound - given[i], max(1, left * loads[i] // whole), spare)
            given[i] = given[i] + more
            spare = spare - more
    return np.array(given)


def gaussian(key, shape, deviation, reach, cuts=(), kind=jnp.bfloat16):
    entries = jax.random.normal(key, shape, jnp.float32) * deviation
    if len(cuts) > 0:
        entries = block_levels(key, shape, cuts, -0.22, 0.18) * entries
    return jnp.clip(entries, min=-reach, max=reach).astype(kind)


def setup_inputs(seed: int = 0) -> dict:
    key_list = jax.random.split(jax.random.key(seed), 14)
    tokens = draw_tokens(jax.random.fold_in(key_list[13], 71), 0)
    spatial_queries = draw_spatial_queries(jax.random.fold_in(key_list[13], 71), 0)
    spatial_keys = draw_spatial_keys(jax.random.fold_in(key_list[13], 71), 0)
    spatial_values = gaussian(key_list[3], (CLIPS, FRAMES, POS, HH), 1.0, 6.0, ((0, 4), (1, 8)))
    spatial_proj = gaussian(key_list[4], (HH, D), HH ** -0.5, 0.1875, ((0, 8),))
    temporal_qkv = draw_temporal_qkv(jax.random.fold_in(key_list[13], 71), 0)
    temporal_proj = gaussian(key_list[6], (HH, D), HH ** -0.5, 0.1875, ((0, 8),))
    frame_mask = draw_frame_mask(jax.random.fold_in(key_list[13], 71), 0)
    expert_ids_keys = jax.random.split(jax.random.fold_in(key_list[8], 1), CLIPS * FRAMES * POS // POS)
    expert_ids_turns = jax.random.permutation(jax.random.fold_in(key_list[8], 3), CLIPS * FRAMES * POS // POS)
    expert_ids = jax.vmap(lambda own, number: deal_out(jax.random.fold_in(key_list[8], 2), own, number, POS, EXPERTS, TOP, CAP, 2))(expert_ids_keys, expert_ids_turns).reshape((CLIPS, FRAMES, POS, TOP))
    gate_values = jnp.clip(0.2 + 0.8 * jax.random.uniform(key_list[9], (CLIPS, FRAMES, POS, TOP), jnp.float32) ** block_levels(key_list[9], (CLIPS, FRAMES, POS, TOP), ((0, 4), (1, 8)), -0.2, 0.2), 0.2, 1.0)
    expert_gate = gaussian(key_list[10], (EXPERTS, D, FF), D ** -0.5, 0.125, ((0, 32),))
    expert_up = gaussian(key_list[11], (EXPERTS, D, FF), D ** -0.5, 0.125, ((0, 32),))
    expert_down = gaussian(key_list[12], (EXPERTS, FF, D), FF ** -0.5, 0.15625, ((0, 32),))
    return {"tokens": tokens, "spatial_queries": spatial_queries, "spatial_keys": spatial_keys, "spatial_values": spatial_values, "spatial_proj": spatial_proj, "temporal_qkv": temporal_qkv, "temporal_proj": temporal_proj, "frame_mask": frame_mask, "expert_ids": expert_ids, "gate_values": gate_values, "expert_gate": expert_gate, "expert_up": expert_up, "expert_down": expert_down}


EPS = 1e-06
MASKED = -1e+30

def rms_normed(values):
    wide = values.astype(jnp.float32)
    inverse = lax.rsqrt(lax.optimization_barrier(jnp.mean(wide * wide, axis=-1, keepdims=True)) + EPS)
    return (wide * inverse).astype(jnp.bfloat16)

def normalize_rows(scores):
    row_max = lax.optimization_barrier(jnp.max(scores, axis=-1, keepdims=True))
    exp_terms = jnp.exp(scores - row_max)
    return (exp_terms / lax.optimization_barrier(jnp.sum(exp_terms, axis=-1, keepdims=True))).astype(jnp.bfloat16)

def spatial_clip(triple):
    queries, keys, values = triple
    score_scale = 1.0 / math.sqrt(HD)
    query_heads = queries.astype(jnp.float32).reshape(FRAMES, POS, HEADS, HD)
    key_heads = keys.astype(jnp.float32).reshape(FRAMES, POS, HEADS, HD)
    value_heads = values.astype(jnp.float32).reshape(FRAMES, POS, HEADS, HD)
    scores = jnp.einsum('fqhd,fkhd->fhqk', query_heads, key_heads) * score_scale
    weights = normalize_rows(scores)
    mixed = jnp.einsum('fhqk,fkhd->fqhd', weights.astype(jnp.float32), value_heads)
    return mixed.astype(jnp.bfloat16).reshape(FRAMES, POS, HEADS * HD)

def reference(tokens, spatial_queries, spatial_keys, spatial_values, spatial_proj, temporal_qkv, temporal_proj, frame_mask, expert_ids, gate_values, expert_gate, expert_up, expert_down):
    score_scale = 1.0 / math.sqrt(HD)
    spatial_mixed = lax.map(spatial_clip, (spatial_queries, spatial_keys, spatial_values))
    spatial_update = jnp.dot(spatial_mixed.reshape(-1, HEADS * HD), spatial_proj, preferred_element_type=jnp.float32)
    first = (tokens.reshape(-1, D).astype(jnp.float32) + spatial_update).astype(jnp.bfloat16)
    normed = rms_normed(first)
    triple = jnp.dot(normed, temporal_qkv, preferred_element_type=jnp.float32).astype(jnp.bfloat16)
    triple = triple.reshape(CLIPS, FRAMES, POS, 3, HEADS, HD).astype(jnp.float32)
    scores = jnp.einsum('ciphd,cjphd->cphij', triple[:, :, :, 0], triple[:, :, :, 1]) * score_scale
    allowed = (frame_mask == 1)[:, None, None, :, :]
    weights = normalize_rows(jnp.where(allowed, scores, MASKED))
    temporal_mixed = jnp.einsum('cphij,cjphd->ciphd', weights.astype(jnp.float32), triple[:, :, :, 2])
    temporal_mixed = temporal_mixed.astype(jnp.bfloat16).reshape(-1, HEADS * HD)
    temporal_update = jnp.dot(temporal_mixed, temporal_proj, preferred_element_type=jnp.float32).astype(jnp.bfloat16)
    second = (first.astype(jnp.float32) + temporal_update.astype(jnp.float32)).astype(jnp.bfloat16)
    routed = rms_normed(second)
    pair_ids = expert_ids.reshape(-1).astype(jnp.int32)
    pair_total = pair_ids.shape[0]
    ordering = jnp.argsort(pair_ids, stable=True).astype(jnp.int32)
    sorted_ids = pair_ids[ordering]
    counts = lax.optimization_barrier(jnp.sum((pair_ids[:, None] == jnp.arange(EXPERTS, dtype=jnp.int32)[None, :]).astype(jnp.int32), axis=0))
    starts = (jnp.cumsum(counts) - counts).astype(jnp.int32)
    rank_sorted = (jnp.arange(pair_total, dtype=jnp.int32) - starts[sorted_ids]).astype(jnp.int32)
    slot_table = jnp.full((EXPERTS, EXPERTS * CAP), -1, jnp.int32).at[sorted_ids, rank_sorted].set(ordering)
    rank_pair = jnp.zeros((pair_total,), jnp.int32).at[ordering].set(rank_sorted)

    def one_expert(pieces):
        pair_index, gate_rows, up_rows, down_rows = pieces
        present = pair_index >= 0
        token_index = (jnp.maximum(pair_index, 0) // TOP).astype(jnp.int32)
        token_rows = jnp.where(present[:, None], routed[token_index], jnp.zeros((), jnp.bfloat16))
        gate_part = jnp.dot(token_rows, gate_rows, preferred_element_type=jnp.float32)
        up_part = jnp.dot(token_rows, up_rows, preferred_element_type=jnp.float32)
        hidden = (jax.nn.silu(gate_part) * up_part).astype(jnp.bfloat16)
        return jnp.dot(hidden, down_rows, preferred_element_type=jnp.float32).astype(jnp.bfloat16)
    answers = lax.map(one_expert, (slot_table, expert_gate, expert_up, expert_down))
    pair_answers = answers[pair_ids, rank_pair].astype(jnp.float32).reshape(-1, TOP, D)
    expert_mix = lax.optimization_barrier(jnp.sum(pair_answers * gate_values.reshape(-1, TOP, 1), axis=1))
    layer_out = (second.astype(jnp.float32) + expert_mix).astype(jnp.bfloat16)
    return layer_out.reshape(CLIPS, FRAMES, POS, D)
```

```python
import math

import jax
import jax.numpy as jnp
from jax import lax
from jax.experimental import pallas as pl
from jax.experimental.pallas import tpu as pltpu
from jax.sharding import PartitionSpec as P


HEADS = 8
HD = 128
TOP = 2


EPS = 1e-06
MASKED = -1e30


def rms_normed(values):
    wide = values.astype(jnp.float32)
    inverse = lax.rsqrt(jnp.mean(wide * wide, axis=-1, keepdims=True) + EPS)
    return (wide * inverse).astype(jnp.bfloat16)


def normalize_rows(scores):
    row_max = jnp.max(scores, axis=-1, keepdims=True)
    exp_terms = jnp.exp(scores - row_max)
    return (exp_terms / jnp.sum(exp_terms, axis=-1, keepdims=True)).astype(jnp.bfloat16)


def add_columns(left_side, piece):
    return jnp.dot(left_side, piece, preferred_element_type=jnp.float32)


def spatial_mix(queries, keys, values):
    positions = queries.shape[0]
    score_scale = 1.0 / math.sqrt(HD)
    query_heads = queries.reshape(positions, HEADS, HD)
    key_heads = keys.reshape(positions, HEADS, HD)
    value_heads = values.reshape(positions, HEADS, HD)
    scores = (
        jnp.einsum("qhd,khd->hqk", query_heads, key_heads, preferred_element_type=jnp.float32)
        * score_scale
    )
    weights = normalize_rows(scores)
    mixed = jnp.einsum("hqk,khd->qhd", weights, value_heads, preferred_element_type=jnp.float32)
    return mixed.astype(jnp.bfloat16).reshape(positions, HEADS * HD)


def temporal_mix(queries, keys, values, allowed):
    frames, positions = (queries.shape[0], queries.shape[1])
    score_scale = 1.0 / math.sqrt(HD)
    query_heads = queries.reshape(frames, positions, HEADS, HD)
    key_heads = keys.reshape(frames, positions, HEADS, HD)
    value_heads = values.reshape(frames, positions, HEADS, HD)
    scores = (
        jnp.einsum("iphd,jphd->phij", query_heads, key_heads, preferred_element_type=jnp.float32)
        * score_scale
    )
    weights = normalize_rows(jnp.where(allowed[None, None, :, :], scores, MASKED))
    mixed = jnp.einsum("phij,jphd->iphd", weights, value_heads, preferred_element_type=jnp.float32)
    return mixed.astype(jnp.bfloat16).reshape(frames, positions, HEADS * HD)


def after(value, *earlier):
    return lax.optimization_barrier((value, *earlier))[0]


def swapped(piece, bit):
    count = lax.axis_size("tm")
    return lax.ppermute(piece, "tm", [(i, i ^ bit) for i in range(count)])


def high_bits():
    count = lax.axis_size("tm")
    return (count // 2, count // 4)


def direct_piece(rows, place):
    return swapped(rows, high_bits()[place])


def far_piece(held, route):
    return swapped(held, high_bits()[1 - route])


def partner_pieces(pieces):
    count = lax.axis_size("clip")
    return [
        lax.ppermute(piece, "clip", [(i, i ^ 1) for i in range(count)]) for piece in pieces
    ]


def all_pieces(rows, direct, far, earlier=()):
    high, low = high_bits()
    pieces = [(0, rows), (high, direct[0]), (low, direct[1]), (high | low, far)]
    bit = low // 2
    while bit:
        pieces = pieces + [
            (offset | bit, swapped(after(piece, *earlier) if earlier else piece, bit))
            for offset, piece in pieces
        ]
        bit //= 2
    return pieces


def times_rows(left_side, pieces, added=None):
    here = lax.axis_index("tm")
    height, width = pieces[0][1].shape
    places = jnp.stack([here ^ offset for offset, _ in pieces]).astype(jnp.int32)
    if height % 128:
        total = None if added is None else added.astype(jnp.float32)
        for number, (_, piece) in enumerate(pieces):
            columns = lax.dynamic_slice_in_dim(left_side, places[number] * height, height, axis=1)
            product = add_columns(columns, piece)
            total = product if total is None else total + product
        total = total.astype(jnp.bfloat16)
        return total if added is None else (total, rms_normed(total))
    extra = [] if added is None else [added]

    def body(places_ref, left_ref, *refs):
        out_refs = refs[len(pieces) + len(extra) :]
        total = None
        for number in range(len(pieces)):
            start = pl.multiple_of(places_ref[number] * height, 128)
            product = jnp.dot(
                left_ref[:, pl.ds(start, height)],
                refs[number][...],
                preferred_element_type=jnp.float32,
            )
            total = product if total is None else total + product
        if extra:
            total = total + refs[len(pieces)][...].astype(jnp.float32)
        rounded = total.astype(jnp.bfloat16)
        out_refs[0][...] = rounded
        if extra:
            out_refs[1][...] = rms_normed(rounded)

    out = jax.ShapeDtypeStruct((left_side.shape[0], width), jnp.bfloat16)
    whole = pl.BlockSpec(memory_space=pltpu.VMEM)
    return pl.pallas_call(
        body,
        out_shape=[out, out] if extra else out,
        in_specs=[pl.BlockSpec(memory_space=pltpu.SMEM)]
        + [whole] * (1 + len(pieces) + len(extra)),
        out_specs=[whole, whole] if extra else whole,
        name="times_rows",
    )(places, left_side, *[piece for _, piece in pieces], *extra)


def expert_rows(blocks, gate, up, down):
    count, model_width = blocks[0].shape
    rows = count * len(blocks)
    width = 512
    while model_width % width:
        width //= 2
    steps = model_width // width
    number = len(blocks)

    def body(*refs):
        ins, (gate_ref, up_ref, down_ref) = refs[:number], refs[number : number + 3]
        outs = refs[number + 3 : 2 * number + 3]
        gate_here, up_here, down_here, all_rows, arrived = refs[2 * number + 3 :]

        def copies(step):
            span = pl.ds(step * width, width)
            return [
                pltpu.make_async_copy(gate_ref.at[span], gate_here.at[span], arrived.at[0, step]),
                pltpu.make_async_copy(up_ref.at[span], up_here.at[span], arrived.at[1, step]),
            ]

        def down_copy(step):
            span = pl.ds(step * width, width)
            return pltpu.make_async_copy(
                down_ref.at[:, span], down_here.at[:, span], arrived.at[2, step]
            )

        for step in range(steps):
            for copy in copies(step):
                copy.start()
        for step in range(steps):
            down_copy(step).start()
        for place, ref in enumerate(ins):
            all_rows[place * count : (place + 1) * count] = ref[...]
        gate_sum = up_sum = None
        for step in range(steps):
            for copy in copies(step):
                copy.wait()
            span = slice(step * width, (step + 1) * width)
            piece = all_rows[:, span]
            gate_part = jnp.dot(piece, gate_here[span], preferred_element_type=jnp.float32)
            up_part = jnp.dot(piece, up_here[span], preferred_element_type=jnp.float32)
            gate_sum = gate_part if gate_sum is None else gate_sum + gate_part
            up_sum = up_part if up_sum is None else up_sum + up_part
        hidden = (jax.nn.silu(gate_sum) * up_sum).astype(jnp.bfloat16)
        for step in range(steps):
            down_copy(step).wait()
            span = slice(step * width, (step + 1) * width)
            answer = jnp.dot(
                hidden, down_here[:, span], preferred_element_type=jnp.float32
            ).astype(jnp.bfloat16)
            for place, ref in enumerate(outs):
                ref[:, span] = answer[place * count : (place + 1) * count]

    whole = pl.BlockSpec(memory_space=pltpu.VMEM)
    return pl.pallas_call(
        body,
        out_shape=[jax.ShapeDtypeStruct(block.shape, jnp.bfloat16) for block in blocks],
        in_specs=[whole] * number + [pl.BlockSpec(memory_space=pl.ANY)] * 3,
        out_specs=[whole] * number,
        scratch_shapes=[
            pltpu.VMEM(gate.shape, jnp.bfloat16),
            pltpu.VMEM(up.shape, jnp.bfloat16),
            pltpu.VMEM(down.shape, jnp.bfloat16),
            pltpu.VMEM((rows, model_width), jnp.bfloat16),
            pltpu.SemaphoreType.DMA((3, steps)),
        ],
        name="expert_rows",
    )(*blocks, gate, up, down)


def packed(wanted, choices, sibling_choices, tokens, sibling_tokens, blocks):
    cap = wanted.shape[0] // blocks

    def body(wanted_ref, choices_ref, sibling_ref, tokens_ref, other_ref, *outs):
        def rows_of(slots, tokens):
            taken = slots[0:1] == wanted_ref[...]
            for k in range(1, TOP):
                taken = taken | (slots[k : k + 1] == wanted_ref[...])
            table = jnp.where(taken, 1.0, 0.0).astype(jnp.bfloat16)
            return jnp.dot(table, tokens[...], preferred_element_type=jnp.float32)

        own = rows_of(choices_ref[...], tokens_ref)
        other = rows_of(sibling_ref[...], other_ref)
        for number, ref in enumerate(outs):
            span = slice(number * cap, (number + 1) * cap)
            ref[...] = jnp.concatenate([own[span], other[span]], axis=0).astype(jnp.bfloat16)

    whole = pl.BlockSpec(memory_space=pltpu.VMEM)
    return pl.pallas_call(
        body,
        out_shape=[jax.ShapeDtypeStruct((2 * cap, tokens.shape[1]), jnp.bfloat16)] * blocks,
        in_specs=[whole] * 5,
        out_specs=[whole] * blocks,
        name="packed",
    )(wanted, choices, sibling_choices, tokens, sibling_tokens)


def weighed(wanted, choices, own_blocks, sibling_blocks, added):
    blocks = len(own_blocks)
    cap = own_blocks[0].shape[0] // 2

    def body(wanted_ref, choices_ref, *refs):
        shares = None
        for k in range(TOP):
            share = jnp.where(
                choices_ref[:, k : k + 1] == wanted_ref[...],
                choices_ref[:, TOP + k : TOP + k + 1],
                0.0,
            )
            shares = share if shares is None else shares + share
        high = shares.astype(jnp.bfloat16)
        low = (shares - high.astype(jnp.float32)).astype(jnp.bfloat16)
        rows = jnp.concatenate(
            [ref[...][:cap] for ref in refs[:blocks]]
            + [ref[...][cap:] for ref in refs[blocks : 2 * blocks]],
            axis=0,
        )
        total = jnp.dot(high, rows, preferred_element_type=jnp.float32)
        total += jnp.dot(low, rows, preferred_element_type=jnp.float32)
        for ref in refs[2 * blocks : -1]:
            total += ref[...].astype(jnp.float32)
        refs[-1][...] = total.astype(jnp.bfloat16)

    whole = pl.BlockSpec(memory_space=pltpu.VMEM)
    return pl.pallas_call(
        body,
        out_shape=jax.ShapeDtypeStruct(
            (choices.shape[0], own_blocks[0].shape[1]), jnp.bfloat16
        ),
        in_specs=[whole] * (2 + 2 * blocks + len(added)),
        out_specs=whole,
        name="weighed",
    )(wanted, choices, *own_blocks, *sibling_blocks, *added)


def over_blocks(blocks):
    return [blocks[0]] + [swapped(block, 2 * k) for k, block in enumerate(blocks) if k]


def ring_step(value, steps=1):
    count = lax.axis_size("clip")
    ring = list(range(0, count, 2)) + sorted(range(1, count, 2), reverse=True)
    return lax.ppermute(
        value, "clip", [(ring[i], ring[(i + steps) % count]) for i in range(count)]
    )


def slots_and_gates(ids, gates, experts, capacity):
    positions = ids.shape[0]
    named = ids.T.reshape(1, TOP * positions)
    chosen = named == jnp.arange(experts, dtype=jnp.int32)[:, None]
    place = jnp.arange(TOP * positions, dtype=jnp.int32)
    before = (place[:, None] < place[None, :]).astype(jnp.bfloat16)
    earlier = jnp.dot(chosen.astype(jnp.bfloat16), before, preferred_element_type=jnp.float32)
    rank = jnp.sum(jnp.where(chosen, earlier, 0.0), axis=0)
    slots = named[0].astype(jnp.float32) * capacity + rank
    return jnp.concatenate([slots.reshape(TOP, positions), gates.T], axis=0)


def wanted_slots(capacity, odd):
    half = lax.axis_size("tm") // 2
    first = lax.axis_index("clip") * 2 * half
    slot = jnp.arange(half * capacity, dtype=jnp.int32)
    expert = first + (lax.axis_index("tm") ^ (2 * (slot // capacity) + odd))
    return (expert * capacity + slot % capacity).astype(jnp.float32)


def layer(
    tokens,
    spatial_queries,
    spatial_keys,
    spatial_values,
    spatial_proj,
    temporal_qkv,
    temporal_proj,
    frame_mask,
    expert_ids,
    gate_values,
    expert_gate,
    expert_up,
    expert_down,
):
    model_width = tokens.shape[3]
    positions = tokens.shape[2]
    tm_count = lax.axis_size("tm")
    clip_count = lax.axis_size("clip")
    experts = clip_count * tm_count
    per_block = positions // tm_count
    resident = tokens.reshape(positions, model_width)
    attended_space = spatial_mix(
        spatial_queries.reshape(positions, -1),
        spatial_keys.reshape(positions, -1),
        spatial_values.reshape(positions, -1),
    )
    third = temporal_qkv.shape[1] // 3
    parity = lax.axis_index("clip") % 2
    half = temporal_proj.shape[1] // 2
    mine, theirs = (
        lax.dynamic_slice_in_dim(temporal_qkv, which * third, third, axis=1)
        for which in (parity, 1 - parity)
    )
    value = temporal_qkv[:, 2 * third :]
    proj_mine, proj_theirs = (
        lax.dynamic_slice_in_dim(temporal_proj, which * half, half, axis=1)
        for which in (parity, 1 - parity)
    )
    spatial_direct = [direct_piece(spatial_proj, place) for place in range(2)]
    spatial_far = far_piece(after(spatial_direct[0], attended_space), 0)
    mine_direct = [direct_piece(after(mine, spatial_direct[0]), 0)]
    mine_direct += [direct_piece(after(mine, spatial_far), 1)]
    value_direct = [direct_piece(after(value, mine_direct[0]), 0)]
    value_direct += [direct_piece(after(value, mine_direct[1]), 1)]
    mine_far = far_piece(mine_direct[1], 1)
    value_far = far_piece(value_direct[0], 0)
    theirs_near = partner_pieces(mine_direct)
    theirs_far = partner_pieces([mine_far])[0]
    capacity = 2 * TOP * positions // experts
    choices = slots_and_gates(
        expert_ids.reshape(positions, TOP), gate_values.reshape(positions, TOP), experts, capacity
    )
    ring_choices = jnp.stack(
        [choices] + [ring_step(choices, step) for step in range(1, clip_count)]
    )
    sibling_choices = swapped(ring_choices, 1)
    turned_choices = jnp.swapaxes(ring_choices, 1, 2)
    even, odd = wanted_slots(capacity, 0), wanted_slots(capacity, 1)
    even_column, both_row = even[:, None], jnp.concatenate([even, odd])[None, :]
    first, normed = times_rows(
        attended_space, all_pieces(spatial_proj, spatial_direct, spatial_far), resident
    )
    allowed = frame_mask[0] == 1
    by_position = lax.all_to_all(
        normed.reshape(tm_count, per_block, model_width),
        "tm",
        split_axis=0,
        concat_axis=0,
        tiled=True,
    )
    frames = by_position.shape[0]
    by_position = after(
        by_position.reshape(frames * per_block, model_width),
        ring_choices,
        sibling_choices,
        turned_choices,
        even_column,
        both_row,
    )
    proj_direct = [
        direct_piece(after(proj_mine, value_direct[place], by_position), place)
        for place in range(2)
    ]

    def projected(*pieces):
        return times_rows(by_position, all_pieces(*pieces, earlier=(by_position,)))

    first_pair = [projected(mine, mine_direct, mine_far), projected(theirs, theirs_near, theirs_far)]
    proj_far = far_piece(after(proj_direct[0], *first_pair), 0)
    proj_near = partner_pieces([after(p, *first_pair) for p in proj_direct])
    values = projected(value, value_direct, value_far)
    proj_partner = partner_pieces([after(proj_far, values)])[0]
    even_plane = parity == 0
    queries = jnp.where(even_plane, first_pair[0], first_pair[1])
    keys = jnp.where(even_plane, first_pair[1], first_pair[0])
    attended_time = temporal_mix(
        *(part.reshape(frames, per_block, third) for part in (queries, keys, values)), allowed
    ).reshape(frames * per_block, third)
    sides = [
        times_rows(attended_time, all_pieces(*pieces, earlier=(values,)))
        for pieces in (
            (proj_mine, proj_direct, proj_far),
            (proj_theirs, proj_near, proj_partner),
        )
    ]
    update_rows = jnp.concatenate(
        [jnp.where(even_plane, sides[0], sides[1]), jnp.where(even_plane, sides[1], sides[0])],
        axis=1,
    )
    returned = lax.all_to_all(
        update_rows.reshape(frames, per_block, model_width),
        "tm",
        split_axis=0,
        concat_axis=0,
        tiled=True,
    )
    temporal_update = returned.reshape(positions, model_width)
    second = (first.astype(jnp.float32) + temporal_update.astype(jnp.float32)).astype(jnp.bfloat16)
    routed = rms_normed(second)
    blocks = tm_count // 2
    experts_here = (expert_gate[0], expert_up[0], expert_down[0])
    received, answers, returned_rows = [], [], []

    def answer(arrived):
        given = expert_rows(arrived, *experts_here)
        answers.append(given[0])
        own = over_blocks(given)
        returned_rows.append((own, [swapped(block, 1) for block in own]))

    def late(arrived, *earlier):
        return [after(arrived[0], *earlier)] + arrived[1:]

    tokens_here = routed
    for step in range(clip_count):
        if step:
            tokens_here = ring_step(tokens_here)
        tokens_now = after(tokens_here, answers[step - 2]) if step > 1 else tokens_here
        sibling_tokens = swapped(tokens_now, 1)
        outgoing = packed(
            even_column,
            ring_choices[step],
            sibling_choices[step],
            tokens_now,
            sibling_tokens,
            blocks,
        )
        received.append(over_blocks(outgoing))
        if step:
            answer(late(received[step - 1], *outgoing))
    carried, carried_here = [], []
    for step in range(1, clip_count):
        if len(returned_rows) == step or step == 2:
            answer(late(received[-1], *carried_here))
        own, other = returned_rows[step]
        carried_here = [weighed(both_row, turned_choices[step], own, other, carried)]
        carried = [ring_step(carried_here[0])]
    layer_out = weighed(both_row, turned_choices[0], *returned_rows[0], [second] + carried)
    return layer_out.reshape(tokens.shape)


def solution(mesh):
    placed = (
        P("clip", "tm", None, None),
        P("clip", "tm", None, None),
        P("clip", "tm", None, None),
        P("clip", "tm", None, None),
        P("tm", None),
        P("tm", None),
        P("tm", None),
        P("clip", None, None),
        P("clip", "tm", None, None),
        P("clip", "tm", None, None),
        P(("clip", "tm"), None, None),
        P(("clip", "tm"), None, None),
        P(("clip", "tm"), None, None),
    )
    return jax.shard_map(
        layer, mesh=mesh, in_specs=placed, out_specs=P("clip", "tm", None, None), check_vma=False
    )
```

```python
import math

import jax
import jax.numpy as jnp
from jax import lax
from jax.experimental import pallas as pl
from jax.experimental.pallas import tpu as pltpu
from jax.sharding import PartitionSpec as P


HEADS = 8
HD = 128
TOP = 2


EPS = 1e-06
MASKED = -1e30


def rms_normed(values):
    wide = values.astype(jnp.float32)
    inverse = lax.rsqrt(jnp.mean(wide * wide, axis=-1, keepdims=True) + EPS)
    return (wide * inverse).astype(jnp.bfloat16)


def normalize_rows(scores):
    row_max = jnp.max(scores, axis=-1, keepdims=True)
    exp_terms = jnp.exp(scores - row_max)
    return (exp_terms / jnp.sum(exp_terms, axis=-1, keepdims=True)).astype(jnp.bfloat16)


def add_columns(left_side, piece):
    return jnp.dot(left_side, piece, preferred_element_type=jnp.float32)


def spatial_mix(queries, keys, values):
    positions = queries.shape[0]
    score_scale = 1.0 / math.sqrt(HD)
    query_heads = queries.reshape(positions, HEADS, HD)
    key_heads = keys.reshape(positions, HEADS, HD)
    value_heads = values.reshape(positions, HEADS, HD)
    scores = (
        jnp.einsum("qhd,khd->hqk", query_heads, key_heads, preferred_element_type=jnp.float32)
        * score_scale
    )
    weights = normalize_rows(scores)
    mixed = jnp.einsum("hqk,khd->qhd", weights, value_heads, preferred_element_type=jnp.float32)
    return mixed.astype(jnp.bfloat16).reshape(positions, HEADS * HD)


def temporal_mix(queries, keys, values, allowed):
    frames, positions = (queries.shape[0], queries.shape[1])
    score_scale = 1.0 / math.sqrt(HD)
    query_heads = queries.reshape(frames, positions, HEADS, HD)
    key_heads = keys.reshape(frames, positions, HEADS, HD)
    value_heads = values.reshape(frames, positions, HEADS, HD)
    scores = (
        jnp.einsum("iphd,jphd->phij", query_heads, key_heads, preferred_element_type=jnp.float32)
        * score_scale
    )
    weights = normalize_rows(jnp.where(allowed[None, None, :, :], scores, MASKED))
    mixed = jnp.einsum("phij,jphd->iphd", weights, value_heads, preferred_element_type=jnp.float32)
    return mixed.astype(jnp.bfloat16).reshape(frames, positions, HEADS * HD)


def after(value, *earlier):
    return lax.optimization_barrier((value, *earlier))[0]


def swapped(piece, bit):
    count = lax.axis_size("tm")
    return lax.ppermute(piece, "tm", [(i, i ^ bit) for i in range(count)])


def high_bits():
    count = lax.axis_size("tm")
    return (count // 2, count // 4)


def direct_piece(rows, place):
    return swapped(rows, high_bits()[place])


def far_piece(held, route):
    return swapped(held, high_bits()[1 - route])


def partner_pieces(pieces):
    count = lax.axis_size("clip")
    return [
        lax.ppermute(piece, "clip", [(i, i ^ 1) for i in range(count)]) for piece in pieces
    ]


def all_pieces(rows, direct, far, earlier=()):
    high, low = high_bits()
    pieces = [(0, rows), (high, direct[0]), (low, direct[1]), (high | low, far)]
    bit = low // 2
    while bit:
        pieces = pieces + [
            (offset | bit, swapped(after(piece, *earlier) if earlier else piece, bit))
            for offset, piece in pieces
        ]
        bit //= 2
    return pieces


def times_rows(left_side, pieces, added=None):
    here = lax.axis_index("tm")
    height, width = pieces[0][1].shape
    places = jnp.stack([here ^ offset for offset, _ in pieces]).astype(jnp.int32)
    if height % 128:
        total = None if added is None else added.astype(jnp.float32)
        for number, (_, piece) in enumerate(pieces):
            columns = lax.dynamic_slice_in_dim(left_side, places[number] * height, height, axis=1)
            product = add_columns(columns, piece)
            total = product if total is None else total + product
        total = total.astype(jnp.bfloat16)
        return total if added is None else (total, rms_normed(total))
    extra = [] if added is None else [added]

    def body(places_ref, left_ref, *refs):
        out_refs = refs[len(pieces) + len(extra) :]
        total = None
        for number in range(len(pieces)):
            start = pl.multiple_of(places_ref[number] * height, 128)
            product = jnp.dot(
                left_ref[:, pl.ds(start, height)],
                refs[number][...],
                preferred_element_type=jnp.float32,
            )
            total = product if total is None else total + product
        if extra:
            total = total + refs[len(pieces)][...].astype(jnp.float32)
        rounded = total.astype(jnp.bfloat16)
        out_refs[0][...] = rounded
        if extra:
            out_refs[1][...] = rms_normed(rounded)

    out = jax.ShapeDtypeStruct((left_side.shape[0], width), jnp.bfloat16)
    whole = pl.BlockSpec(memory_space=pltpu.VMEM)
    return pl.pallas_call(
        body,
        out_shape=[out, out] if extra else out,
        in_specs=[pl.BlockSpec(memory_space=pltpu.SMEM)]
        + [whole] * (1 + len(pieces) + len(extra)),
        out_specs=[whole, whole] if extra else whole,
        compiler_params=pltpu.CompilerParams(vmem_limit_bytes=20 * 2**20),
        name="times_rows",
    )(places, left_side, *[piece for _, piece in pieces], *extra)


def expert_rows(blocks, gate, up, down):
    count, model_width = blocks[0].shape
    rows = count * len(blocks)
    hidden_width = gate.shape[1]
    width = 1024
    while model_width % width:
        width //= 2
    steps = model_width // width

    def body(*refs):
        ins, (gate_ref, up_ref, down_ref) = refs[: len(blocks)], refs[len(blocks) : len(blocks) + 3]
        outs = refs[len(blocks) + 3 : 2 * len(blocks) + 3]
        gate_sum, up_sum, hidden = refs[2 * len(blocks) + 3 :]
        step = pl.program_id(0)

        @pl.when(step < steps)
        def _():
            piece = jnp.concatenate([ref[...] for ref in ins], axis=0)
            gate_part = jnp.dot(piece, gate_ref[...], preferred_element_type=jnp.float32)
            up_part = jnp.dot(piece, up_ref[...], preferred_element_type=jnp.float32)

            @pl.when(step == 0)
            def _():
                gate_sum[...] = gate_part
                up_sum[...] = up_part

            if steps > 2:

                @pl.when((step > 0) & (step < steps - 1))
                def _():
                    gate_sum[...] += gate_part
                    up_sum[...] += up_part

            @pl.when(step == steps - 1)
            def _():
                total = gate_part if steps == 1 else gate_sum[...] + gate_part
                above = up_part if steps == 1 else up_sum[...] + up_part
                hidden[...] = (jax.nn.silu(total) * above).astype(jnp.bfloat16)

        @pl.when(step >= steps)
        def _():
            answer = jnp.dot(
                hidden[...], down_ref[...], preferred_element_type=jnp.float32
            ).astype(jnp.bfloat16)
            for number, ref in enumerate(outs):
                ref[...] = answer[number * count : (number + 1) * count]

    return pl.pallas_call(
        body,
        grid=(2 * steps,),
        out_shape=[jax.ShapeDtypeStruct(block.shape, jnp.bfloat16) for block in blocks],
        in_specs=[pl.BlockSpec((count, width), lambda i: (0, jnp.minimum(i, steps - 1)))]
        * len(blocks)
        + [
            pl.BlockSpec((width, hidden_width), lambda i: (jnp.minimum(i, steps - 1), 0)),
            pl.BlockSpec((width, hidden_width), lambda i: (jnp.minimum(i, steps - 1), 0)),
            pl.BlockSpec((hidden_width, width), lambda i: (0, jnp.maximum(i - steps, 0))),
        ],
        out_specs=[pl.BlockSpec((count, width), lambda i: (0, jnp.maximum(i - steps, 0)))]
        * len(blocks),
        scratch_shapes=[
            pltpu.VMEM((rows, hidden_width), jnp.float32),
            pltpu.VMEM((rows, hidden_width), jnp.float32),
            pltpu.VMEM((rows, hidden_width), jnp.bfloat16),
        ],
        compiler_params=pltpu.CompilerParams(vmem_limit_bytes=28 * 2**20),
        name="expert_rows",
    )(*blocks, gate, up, down)


def packed(wanted, choices, sibling_choices, tokens, sibling_tokens, blocks):
    cap = wanted.shape[0] // blocks

    def body(wanted_ref, choices_ref, sibling_ref, tokens_ref, other_ref, *outs):
        def rows_of(slots, tokens):
            taken = slots[0:1] == wanted_ref[...]
            for k in range(1, TOP):
                taken = taken | (slots[k : k + 1] == wanted_ref[...])
            table = jnp.where(taken, 1.0, 0.0).astype(jnp.bfloat16)
            return jnp.dot(table, tokens[...], preferred_element_type=jnp.float32)

        own = rows_of(choices_ref[...], tokens_ref)
        other = rows_of(sibling_ref[...], other_ref)
        for number, ref in enumerate(outs):
            span = slice(number * cap, (number + 1) * cap)
            ref[...] = jnp.concatenate([own[span], other[span]], axis=0).astype(jnp.bfloat16)

    whole = pl.BlockSpec(memory_space=pltpu.VMEM)
    return pl.pallas_call(
        body,
        out_shape=[jax.ShapeDtypeStruct((2 * cap, tokens.shape[1]), jnp.bfloat16)] * blocks,
        in_specs=[whole] * 5,
        out_specs=[whole] * blocks,
        compiler_params=pltpu.CompilerParams(vmem_limit_bytes=14 * 2**20),
        name="packed",
    )(wanted, choices, sibling_choices, tokens, sibling_tokens)


def weighed(wanted, choices, own_blocks, sibling_blocks, added, kind):
    blocks = len(own_blocks)
    cap = own_blocks[0].shape[0] // 2

    def body(wanted_ref, choices_ref, *refs):
        shares = None
        for k in range(TOP):
            share = jnp.where(
                choices_ref[:, k : k + 1] == wanted_ref[...],
                choices_ref[:, TOP + k : TOP + k + 1],
                0.0,
            )
            shares = share if shares is None else shares + share
        high = shares.astype(jnp.bfloat16)
        low = (shares - high.astype(jnp.float32)).astype(jnp.bfloat16)
        rows = jnp.concatenate(
            [ref[...][:cap] for ref in refs[:blocks]]
            + [ref[...][cap:] for ref in refs[blocks : 2 * blocks]],
            axis=0,
        )
        total = jnp.dot(high, rows, preferred_element_type=jnp.float32)
        total += jnp.dot(low, rows, preferred_element_type=jnp.float32)
        for ref in refs[2 * blocks : -1]:
            total += ref[...].astype(jnp.float32)
        refs[-1][...] = total.astype(kind)

    whole = pl.BlockSpec(memory_space=pltpu.VMEM)
    return pl.pallas_call(
        body,
        out_shape=jax.ShapeDtypeStruct((choices.shape[0], own_blocks[0].shape[1]), kind),
        in_specs=[whole] * (2 + 2 * blocks + len(added)),
        out_specs=whole,
        compiler_params=pltpu.CompilerParams(vmem_limit_bytes=14 * 2**20),
        name="weighed",
    )(wanted, choices, *own_blocks, *sibling_blocks, *added)


def over_blocks(blocks):
    return [blocks[0]] + [swapped(block, 2 * k) for k, block in enumerate(blocks) if k]


def ring_step(value, steps=1):
    count = lax.axis_size("clip")
    ring = list(range(0, count, 2)) + sorted(range(1, count, 2), reverse=True)
    return lax.ppermute(
        value, "clip", [(ring[i], ring[(i + steps) % count]) for i in range(count)]
    )


def slots_and_gates(ids, gates, experts, capacity):
    positions = ids.shape[0]
    named = ids.T.reshape(1, TOP * positions)
    chosen = named == jnp.arange(experts, dtype=jnp.int32)[:, None]
    place = jnp.arange(TOP * positions, dtype=jnp.int32)
    before = (place[:, None] < place[None, :]).astype(jnp.bfloat16)
    earlier = jnp.dot(chosen.astype(jnp.bfloat16), before, preferred_element_type=jnp.float32)
    rank = jnp.sum(jnp.where(chosen, earlier, 0.0), axis=0)
    slots = named[0].astype(jnp.float32) * capacity + rank
    return jnp.concatenate([slots.reshape(TOP, positions), gates.T], axis=0)


def wanted_slots(capacity, odd):
    half = lax.axis_size("tm") // 2
    first = lax.axis_index("clip") * 2 * half
    slot = jnp.arange(half * capacity, dtype=jnp.int32)
    expert = first + (lax.axis_index("tm") ^ (2 * (slot // capacity) + odd))
    return (expert * capacity + slot % capacity).astype(jnp.float32)


def layer(
    tokens,
    spatial_queries,
    spatial_keys,
    spatial_values,
    spatial_proj,
    temporal_qkv,
    temporal_proj,
    frame_mask,
    expert_ids,
    gate_values,
    expert_gate,
    expert_up,
    expert_down,
):
    model_width = tokens.shape[3]
    positions = tokens.shape[2]
    tm_count = lax.axis_size("tm")
    clip_count = lax.axis_size("clip")
    experts = clip_count * tm_count
    per_block = positions // tm_count
    resident = tokens.reshape(positions, model_width)
    attended_space = spatial_mix(
        spatial_queries.reshape(positions, -1),
        spatial_keys.reshape(positions, -1),
        spatial_values.reshape(positions, -1),
    )
    third = temporal_qkv.shape[1] // 3
    parity = lax.axis_index("clip") % 2
    half = temporal_proj.shape[1] // 2
    mine, theirs = (
        lax.dynamic_slice_in_dim(temporal_qkv, which * third, third, axis=1)
        for which in (parity, 1 - parity)
    )
    value = temporal_qkv[:, 2 * third :]
    proj_mine, proj_theirs = (
        lax.dynamic_slice_in_dim(temporal_proj, which * half, half, axis=1)
        for which in (parity, 1 - parity)
    )
    spatial_direct = [direct_piece(spatial_proj, place) for place in range(2)]
    spatial_far = far_piece(after(spatial_direct[0], attended_space), 0)
    mine_direct = [direct_piece(after(mine, spatial_direct[0]), 0)]
    mine_direct += [direct_piece(after(mine, spatial_far), 1)]
    value_direct = [direct_piece(after(value, mine_direct[0]), 0)]
    value_direct += [direct_piece(after(value, mine_direct[1]), 1)]
    mine_far = far_piece(mine_direct[1], 1)
    value_far = far_piece(value_direct[0], 0)
    theirs_near = partner_pieces(mine_direct)
    theirs_far = partner_pieces([mine_far])[0]
    capacity = 2 * TOP * positions // experts
    choices = slots_and_gates(
        expert_ids.reshape(positions, TOP), gate_values.reshape(positions, TOP), experts, capacity
    )
    ring_choices = jnp.stack(
        [choices] + [ring_step(choices, step) for step in range(1, clip_count)]
    )
    sibling_choices = swapped(ring_choices, 1)
    turned_choices = jnp.swapaxes(ring_choices, 1, 2)
    even, odd = wanted_slots(capacity, 0), wanted_slots(capacity, 1)
    even_column, both_row = even[:, None], jnp.concatenate([even, odd])[None, :]
    first, normed = times_rows(
        attended_space, all_pieces(spatial_proj, spatial_direct, spatial_far), resident
    )
    allowed = frame_mask[0] == 1
    by_position = lax.all_to_all(
        normed.reshape(tm_count, per_block, model_width),
        "tm",
        split_axis=0,
        concat_axis=0,
        tiled=True,
    )
    frames = by_position.shape[0]
    by_position = after(
        by_position.reshape(frames * per_block, model_width),
        ring_choices,
        sibling_choices,
        turned_choices,
        even_column,
        both_row,
    )
    proj_direct = [direct_piece(after(proj_mine, mine_direct[place]), place) for place in range(2)]

    def projected(*pieces):
        return times_rows(by_position, all_pieces(*pieces, earlier=(by_position,)))

    first_pair = [projected(mine, mine_direct, mine_far), projected(theirs, theirs_near, theirs_far)]
    proj_far = far_piece(after(proj_direct[0], by_position), 0)
    proj_near = partner_pieces([after(p, by_position) for p in proj_direct])
    values = projected(value, value_direct, value_far)
    proj_partner = partner_pieces([after(proj_far, first_pair[0])])[0]
    even_plane = parity == 0
    queries = jnp.where(even_plane, first_pair[0], first_pair[1])
    keys = jnp.where(even_plane, first_pair[1], first_pair[0])
    attended_time = temporal_mix(
        *(part.reshape(frames, per_block, third) for part in (queries, keys, values)), allowed
    ).reshape(frames * per_block, third)
    sides = [
        times_rows(attended_time, all_pieces(*pieces, earlier=(values,)))
        for pieces in (
            (proj_mine, proj_direct, proj_far),
            (proj_theirs, proj_near, proj_partner),
        )
    ]
    update_rows = jnp.concatenate(
        [jnp.where(even_plane, sides[0], sides[1]), jnp.where(even_plane, sides[1], sides[0])],
        axis=1,
    )
    returned = lax.all_to_all(
        update_rows.reshape(frames, per_block, model_width),
        "tm",
        split_axis=0,
        concat_axis=0,
        tiled=True,
    )
    temporal_update = returned.reshape(positions, model_width)
    second = (first.astype(jnp.float32) + temporal_update.astype(jnp.float32)).astype(jnp.bfloat16)
    routed = rms_normed(second)
    blocks = tm_count // 2
    experts_here = (expert_gate[0], expert_up[0], expert_down[0])
    received, answers, returned_rows = [], [], []

    def answer(arrived):
        given = expert_rows(arrived, *experts_here)
        answers.append(given[0])
        own = over_blocks(given)
        returned_rows.append((own, [swapped(block, 1) for block in own]))

    def late(arrived, *earlier):
        return [after(arrived[0], *earlier)] + arrived[1:]

    def give(step, tokens_now):
        sibling_tokens = swapped(tokens_now, 1)
        outgoing = packed(
            even_column,
            ring_choices[step],
            sibling_choices[step],
            tokens_now,
            sibling_tokens,
            blocks,
        )
        received.append(over_blocks(outgoing))

    def weigh(step, added, kind):
        return weighed(
            both_row, turned_choices[step], *returned_rows[step], added, kind
        )

    circling = [routed]
    for _ in range(1, clip_count):
        circling.append(ring_step(circling[-1]))
    give(0, circling[0])
    give(1, circling[1])
    answer(late(received[0], received[1][0]))
    answer(late(received[1], answers[0]))
    if clip_count > 2:
        give(2, after(circling[2], answers[1]))
    total = first_mix = weigh(1, [], jnp.bfloat16)
    for step in range(3, clip_count):
        give(step, after(circling[step], first_mix))
    for step in range(2, clip_count):
        answer(late(received[step], answers[step - 1], received[-1][0]))
    for step in range(1, clip_count):
        if step == 2:
            total = weigh(step, [carried], jnp.bfloat16)
        elif step > 2:
            part = weigh(step, [], jnp.float32)
            total = (carried.astype(jnp.float32) + part).astype(jnp.bfloat16)
        carried = ring_step(total)
    own_part = weigh(0, [second], jnp.float32)
    layer_out = (own_part + carried.astype(jnp.float32)).astype(jnp.bfloat16)
    return layer_out.reshape(tokens.shape)


def solution(mesh):
    placed = (
        P("clip", "tm", None, None),
        P("clip", "tm", None, None),
        P("clip", "tm", None, None),
        P("clip", "tm", None, None),
        P("tm", None),
        P("tm", None),
        P("tm", None),
        P("clip", None, None),
        P("clip", "tm", None, None),
        P("clip", "tm", None, None),
        P(("clip", "tm"), None, None),
        P(("clip", "tm"), None, None),
        P(("clip", "tm"), None, None),
    )
    return jax.shard_map(
        layer, mesh=mesh, in_specs=placed, out_specs=P("clip", "tm", None, None), check_vma=False
    )
```
